32 devices in a mesh: row: 8 (over y, x, core), col: 4 (over z).
Axes of the slice: x: 2, y: 2, z: 4, core: 2. Of those that a mesh axis runs over, the one named last changes fastest.
Arguments:
- singular_vectors: float32 [4096, 4096], P('row', 'col'), may hold values from -6 to 6
- reflector_vectors: float32 [2, 16, 256, 512], P(None, 'row', 'col'), may hold values from -2 to 2, as said below
- reflector_factors: float32 [2, 16, 256, 256], P(None, 'row', 'col'), as said below
- sweep_bounds: int32 [2, 2], replicated, may hold values from 0 to 3584, as said below
Outputs:
- transformed: float32 [4096, 4096], P('row', 'col')
The draws below stay inside these ranges and needn't reach their ends.
Inputs may be any that keep to these rules, and one draw needn't show every extreme that they name: `reflector_vectors`: row j of each block's 256 x 2 * 256 slice is a reflector: 1 at position j, nonzero only at positions j to j + 255. `reflector_factors`: each block's factor is the upper triangular inverse of the strictly upper part of W W^T plus half of its diagonal, W being that block's slice of reflector_vectors, so that each block's transformation is orthogonal. `sweep_bounds`: both entries are multiples of 256, and the first is below the second.
All inputs are finite; a program needn't handle non-finite values.
Results may differ from the reference program's by a relative error of at most 0.0003.
Values sent between devices are 32-bit elements; how exact they have to be, the bound alone decides.
A program may use at most 64 MiB of HBM per device.

```python
import jax
import jax.numpy as jnp
from jax import lax

BW = 256
NV = 4096
SWEEPS = 2
ROWS = 4096
BLOCKS = 16


exact_mode = lax.Precision.HIGHEST


def build_factor(vectors):
    gram = jnp.dot(vectors, vectors.T, precision=exact_mode, preferred_element_type=jnp.float32)
    upper = jnp.triu(gram, 1) + jnp.diag(0.5 * jnp.diagonal(gram))
    identity = jnp.eye(gram.shape[0], dtype=jnp.float32)
    return lax.linalg.triangular_solve(upper, identity, left_side=True, lower=False)


def reflector_pair(key):
    base_key = jax.random.fold_in(key, 11)
    tail_scale = 0.25 / BW ** 0.5
    noise = jax.random.truncated_normal(base_key, -4.0, 4.0, (SWEEPS, BLOCKS, BW, 2 * BW), jnp.float32)
    column = lax.broadcasted_iota(jnp.int32, (BW, 2 * BW), 1)
    reflector_row = lax.broadcasted_iota(jnp.int32, (BW, 2 * BW), 0)
    tail_mask = (column > reflector_row) & (column < reflector_row + BW)
    head_mask = column == reflector_row
    far_mask = column == reflector_row + BW - 1
    vectors = jnp.where(tail_mask, noise * tail_scale, 0.0) + jnp.where(head_mask, 1.0, 0.0) + jnp.where(far_mask, 1.0, 0.0)
    vectors = vectors.astype(jnp.float32)
    factors = jax.vmap(jax.vmap(build_factor))(vectors)
    return (vectors, factors)


def draw_reflector_vectors(key, part):
    return reflector_pair(key)[0]


def draw_reflector_factors(key, part):
    return reflector_pair(key)[1]


def draw_sweep_bounds(key, part):
    first_key = jax.random.fold_in(key, 21)
    last_key = jax.random.fold_in(key, 22)
    first_row = jax.random.randint(first_key, (SWEEPS,), 0, BLOCKS // 4) * BW
    last_row = jax.random.randint(last_key, (SWEEPS,), BLOCKS * 3 // 4 - 1, BLOCKS - 1) * BW
    return jnp.stack([first_row, last_row], axis=1).astype(jnp.int32)


def steps_of(own_key, dims, pieces, smallest, largest):
    level, own = 1.0, jax.random.fold_in(own_key, 6)
    for axis_at, shards_of in pieces:
        heights = jnp.exp(jax.random.uniform(jax.random.fold_in(own, axis_at), (shards_of,), jnp.float32, smallest / len(pieces), largest / len(pieces)))
        level = level * jnp.repeat(heights, dims[axis_at] // shards_of).reshape([-1 if axis == axis_at else 1 for axis in range(len(dims))])
    return level


def centred(stream_key, shape, deviation, most, pieces=(), held_as=jnp.bfloat16):
    array = jax.random.normal(stream_key, shape, jnp.float32) * deviation
    if len(pieces) > 0:
        array = steps_of(stream_key, shape, pieces, -0.22, 0.18) * array
    return jnp.clip(array, min=-most, max=most).astype(held_as)


def setup_inputs(seed: int = 0) -> dict:
    arg_keys = jax.random.split(jax.random.key(seed), 5)
    return {
        "singular_vectors": centred(arg_keys[0], (ROWS, NV), 1.0, 6.0, ((0, 8), (1, 4)), jnp.float32),
        "reflector_vectors": draw_reflector_vectors(jax.random.fold_in(arg_keys[4], 71), 0),
        "reflector_factors": draw_reflector_factors(jax.random.fold_in(arg_keys[4], 71), 0),
        "sweep_bounds": draw_sweep_bounds(jax.random.fold_in(arg_keys[4], 71), 0),
    }


exact_mode = lax.Precision.HIGHEST

def apply_block(row_block, vectors, factor):
    inner_part = jnp.dot(vectors.astype(jnp.float32), row_block.astype(jnp.float32), precision=exact_mode, preferred_element_type=jnp.float32)
    inner_part = jnp.dot(factor.astype(jnp.float32), inner_part.astype(jnp.float32), precision=exact_mode, preferred_element_type=jnp.float32)
    return row_block - jnp.dot(vectors.T.astype(jnp.float32), inner_part.astype(jnp.float32), precision=exact_mode, preferred_element_type=jnp.float32)

def keep_same(matrix):
    return matrix

def reference(singular_vectors, reflector_vectors, reflector_factors, sweep_bounds):

    def one_sweep(field_now, sweep_id):
        first_row = sweep_bounds[sweep_id, 0]
        last_row = sweep_bounds[sweep_id, 1]

        def one_block(counter, current):
            block_id = (BLOCKS - 1 - counter).astype(jnp.int32)
            start_row = (block_id * BW).astype(jnp.int32)
            is_live = (start_row >= first_row) & (start_row <= last_row)

            def update(matrix):
                row_block = lax.dynamic_slice_in_dim(matrix, start_row, 2 * BW, 0)
                row_block = apply_block(row_block, reflector_vectors[sweep_id, block_id], reflector_factors[sweep_id, block_id])
                return lax.dynamic_update_slice_in_dim(matrix, row_block, start_row, 0)
            return lax.cond(is_live, update, keep_same, current)
        return (lax.fori_loop(0, BLOCKS, one_block, field_now), None)
    result_field, unused = lax.scan(one_sweep, singular_vectors, jnp.arange(SWEEPS, dtype=jnp.int32))
    return result_field
```

```python
import functools

import jax
import jax.numpy as jnp
from jax import lax
from jax.experimental import pallas as pl
from jax.experimental.pallas import tpu as pltpu
from jax.sharding import PartitionSpec as P

MESH = pl.DeviceIdType.MESH
f32, bf16 = jnp.float32, jnp.bfloat16
WIDTH = 128


def split(value):
    high = value.astype(bf16)
    return high, (value - high.astype(f32)).astype(bf16)


def dot3(a_high, a_low, b):
    b_high, b_low = split(b)
    dot = functools.partial(jnp.dot, preferred_element_type=f32)
    return dot(a_high, b_high) + (dot(a_high, b_low) + dot(a_low, b_high))


def kernel(
    count, x_ref, w_ref, out_ref,
    g_high, g_low, v_high, v_low, from_s0, from_s1, to_s0, to_s1, final,
    up_send, up_recv, down_send, down_recv,
):
    me = lax.axis_index("row")
    bw = g_high.shape[1]
    pieces, width = from_s0.shape[0], from_s0.shape[2]

    barrier = pltpu.get_barrier_semaphore()

    @pl.when(me > 0)
    def _():
        pl.semaphore_signal(barrier, inc=1, device_id={"row": me - 1}, device_id_type=MESH)

    @pl.when(me < count - 1)
    def _():
        pl.semaphore_signal(barrier, inc=1, device_id={"row": me + 1}, device_id_type=MESH)

    peers = jnp.where(me > 0, 1, 0) + jnp.where(me < count - 1, 1, 0)
    pl.semaphore_wait(barrier, peers)

    def prepare(k, carry):
        w_t = w_ref[k, :, : 2 * bw]
        f_high, f_low = split(w_ref[k, :, 2 * bw :])
        high, low = split(dot3(f_high, f_low, w_t))
        g_high[k], g_low[k] = high, low
        high, low = split(w_t.T)
        v_high[k], v_low[k] = high, low
        return carry

    lax.fori_loop(0, g_high.shape[0], prepare, 0)

    def apply(k, top, bottom):
        inner = dot3(g_high[k], g_low[k], jnp.concatenate([top, bottom], axis=0))
        change = dot3(v_high[k], v_low[k], inner)
        return top - change[:bw], bottom - change[bw:]

    def up(s, p):
        source, target = ((to_s0, from_s0), (to_s1, from_s1))[s]
        return pltpu.make_async_remote_copy(
            src_ref=source.at[p], dst_ref=target.at[p],
            send_sem=up_send.at[s, p], recv_sem=up_recv.at[s, p],
            device_id={"row": me - 1}, device_id_type=MESH,
        )

    def columns(p):
        return pl.ds(pl.multiple_of(p * width, width), width)

    def down(p):
        return pltpu.make_async_remote_copy(
            src_ref=final.at[p], dst_ref=out_ref.at[:, columns(p)],
            send_sem=down_send.at[p], recv_sem=down_recv.at[p],
            device_id={"row": me + 1}, device_id_type=MESH,
        )

    @pl.when(me == count - 1)
    def _():
        def piece(p, carry):
            x0, x1 = apply(1, x_ref[:bw, columns(p)], x_ref[bw:, columns(p)])
            to_s0[p] = x0
            up(0, p).start()
            to_s1[p] = x1
            up(1, p).start()
            return carry

        lax.fori_loop(0, pieces, piece, 0)

    @pl.when(me < count - 1)
    def _():
        def piece(p, carry):
            up(0, p).wait_recv()
            x1, b0 = apply(0, x_ref[bw:, columns(p)], from_s0[p])
            x0, x1 = apply(1, x_ref[:bw, columns(p)], x1)
            to_s0[p] = x0

            @pl.when(me > 0)
            def _():
                up(0, p).start()

            up(1, p).wait_recv()
            b0, b1 = apply(2, b0, from_s1[p])
            x1, b0 = apply(3, x1, b0)
            to_s1[p] = x1

            @pl.when(me > 0)
            def _():
                up(1, p).start()

            final[p, :bw] = b0
            final[p, bw:] = b1
            down(p).start()

            @pl.when(me == 0)
            def _():
                top, bottom = apply(4, to_s0[p], to_s1[p])
                out_ref[:bw, columns(p)] = top
                out_ref[bw:, columns(p)] = bottom

            return carry

        lax.fori_loop(0, pieces, piece, 0)

    def finish(p, carry):
        @pl.when(me > 0)
        def _():
            up(0, p).wait_send()
            up(1, p).wait_send()
            down(p).wait_recv()

        @pl.when(me < count - 1)
        def _():
            down(p).wait_send()

        return carry

    lax.fori_loop(0, pieces, finish, 0)


def per_device(singular_vectors, reflector_vectors, reflector_factors, sweep_bounds):
    count = lax.axis_size("row")
    me = lax.axis_index("row")
    rows, cols = singular_vectors.shape
    sweeps, blocks, _, span = reflector_vectors.shape
    bw = span // 2
    assert sweeps == 2 and blocks == 2 and rows == span and cols % WIDTH == 0
    pieces = cols // WIDTH

    both = jnp.concatenate([reflector_vectors, reflector_factors], axis=3)
    start = (me * blocks + jnp.arange(blocks)) * bw
    live = (start[None] >= sweep_bounds[:, :1]) & (start[None] <= sweep_bounds[:, 1:])
    is_factor = jnp.arange(span + bw) >= span
    both = jnp.where(live[:, :, None, None] | ~is_factor, both, 0.0)
    below = lax.ppermute(both[1, 0], "row", [(i + 1, i) for i in range(count - 1)])
    stack = jnp.stack([both[0, 1], both[0, 0], below, both[1, 1], both[1, 0]])
    weights = lax.all_gather(stack, "col", axis=1, tiled=True)

    n = weights.shape[0]
    piece = pltpu.VMEM((pieces, bw, WIDTH), f32)
    return pl.pallas_call(
        functools.partial(kernel, count),
        out_shape=jax.ShapeDtypeStruct((rows, cols), f32),
        in_specs=[pl.BlockSpec(memory_space=pltpu.VMEM)] * 2,
        out_specs=pl.BlockSpec(memory_space=pltpu.VMEM),
        scratch_shapes=[
            pltpu.VMEM((n, bw, span), bf16),
            pltpu.VMEM((n, bw, span), bf16),
            pltpu.VMEM((n, span, bw), bf16),
            pltpu.VMEM((n, span, bw), bf16),
            piece, piece, piece, piece,
            pltpu.VMEM((pieces, span, WIDTH), f32),
            pltpu.SemaphoreType.DMA((2, pieces)),
            pltpu.SemaphoreType.DMA((2, pieces)),
            pltpu.SemaphoreType.DMA((pieces,)),
            pltpu.SemaphoreType.DMA((pieces,)),
        ],
        compiler_params=pltpu.CompilerParams(
            collective_id=0, has_side_effects=True, vmem_limit_bytes=56 * 2**20
        ),
    )(singular_vectors, weights)


def solution(mesh):
    placed = (P("row", "col"), P(None, "row", "col", None), P(None, "row", "col", None), P())
    return jax.shard_map(
        per_device, mesh=mesh, in_specs=placed, out_specs=P("row", "col"), check_vma=False
    )
```

```python
import functools

import jax
import jax.numpy as jnp
from jax import lax
from jax.experimental import pallas as pl
from jax.experimental.pallas import tpu as pltpu
from jax.sharding import PartitionSpec as P

MESH = pl.DeviceIdType.MESH
f32, bf16 = jnp.float32, jnp.bfloat16
WIDTH = 128


def split(value):
    high = value.astype(bf16)
    return high, (value - high.astype(f32)).astype(bf16)


def dot3(a, b):
    (a_high, a_low), (b_high, b_low) = a, b
    dot = functools.partial(jnp.dot, preferred_element_type=f32)
    return dot(a_high, b_high) + (dot(a_high, b_low) + dot(a_low, b_high))


def kernel(
    count, ring, bounds_ref, x_ref, vec_ref, fac_ref, out_ref,
    gathered, upper_high, upper_low, lower_high, lower_low,
    below, tops, returned, back, middle,
    hop_send, hop_recv, far_send, far_recv, up_send, up_recv, down_send, down_recv,
):
    me, slab = lax.axis_index("row"), lax.axis_index("col")
    bw = gathered.shape[2]
    part = bw // ring
    pieces, width = below.shape[1], below.shape[3]
    first, last = me == 0, me == count - 1

    def block_rows(owner):
        return pl.ds(pl.multiple_of(owner * part, part), part)

    for s in range(2):
        for b in range(2):
            w = vec_ref[s, b]
            gathered[s, b, block_rows(slab), :bw] = w[:, :bw] + w[:, bw:]
            gathered[s, b, block_rows(slab), bw:] = fac_ref[s, b]

    @pl.when(last)
    def _():
        below[...] = jnp.zeros_like(below)

    barrier = pltpu.get_barrier_semaphore()

    @pl.when(jnp.logical_not(first))
    def _():
        pl.semaphore_signal(barrier, inc=1, device_id={"row": me - 1}, device_id_type=MESH)

    @pl.when(jnp.logical_not(last))
    def _():
        pl.semaphore_signal(barrier, inc=1, device_id={"row": me + 1}, device_id_type=MESH)

    for k in range(1, ring):
        pl.semaphore_signal(
            barrier, inc=1, device_id={"col": lax.rem(slab + k, ring)}, device_id_type=MESH
        )
    peers = jnp.where(me > 0, 1, 0) + jnp.where(me < count - 1, 1, 0) + ring - 1
    pl.semaphore_wait(barrier, peers)

    def hop(way, t, owner):
        block = gathered.at[0, :, block_rows(owner)]
        return pltpu.make_async_remote_copy(
            src_ref=block, dst_ref=block,
            send_sem=hop_send.at[way, t], recv_sem=hop_recv.at[way, t],
            device_id={"col": slab + (1 - 2 * way)}, device_id_type=MESH,
        )

    def sends(way, t):
        if way == 0:
            return (slab - t >= 0) & (slab + 1 < ring)
        return (slab + t < ring) & (slab >= 1)

    def gets(way, t):
        return slab - 1 - t >= 0 if way == 0 else slab + 1 + t < ring

    for t in range(ring - 1):
        for way in range(2):
            sign = 1 - 2 * way

            @pl.when(sends(way, t))
            def _():
                hop(way, t, slab - sign * t).start()

        for way in range(2):
            sign = 1 - 2 * way

            @pl.when(gets(way, t))
            def _():
                hop(way, t, slab - sign * (t + 1)).wait_recv()

    def far(k, owner):
        block = gathered.at[1, :, block_rows(owner)]
        return pltpu.make_async_remote_copy(
            src_ref=block, dst_ref=block,
            send_sem=far_send.at[k], recv_sem=far_recv.at[k],
            device_id={"col": lax.rem(slab + k, ring)}, device_id_type=MESH,
        )

    for k in range(1, ring):
        far(k, slab).start()

    def build(s):
        row = lax.broadcasted_iota(jnp.int32, (bw, bw), 0)
        col = lax.broadcasted_iota(jnp.int32, (bw, bw), 1)
        row2 = lax.broadcasted_iota(jnp.int32, (2 * bw, 2 * bw), 0)
        col2 = lax.broadcasted_iota(jnp.int32, (2 * bw, 2 * bw), 1)
        unit = jnp.where(row2 == col2, 1.0, 0.0).astype(f32)

        def whole(b):
            start = (me * 2 + b) * bw
            live = (start >= bounds_ref[s, 0]) & (start <= bounds_ref[s, 1])
            packed = gathered[s, b, :, :bw]
            factor = gathered[s, b, :, bw:] * jnp.where(live, 1.0, 0.0).astype(f32)
            w_t = jnp.concatenate(
                [jnp.where(col >= row, packed, 0.0), jnp.where(col < row, packed, 0.0)], axis=1
            )
            g = dot3(split(factor), split(w_t))
            return unit - dot3(split(w_t.T), split(g))

        q1 = whole(1)
        lower_high[s], lower_low[s] = split(q1[bw:])
        q0 = whole(0)
        mixed = dot3(split(q0[:, bw:]), split(q1[:bw]))
        upper_high[s, :, :bw], upper_low[s, :, :bw] = split(q0[:, :bw])
        upper_high[s, :, bw:], upper_low[s, :, bw:] = split(mixed)

    def columns(p):
        return pl.ds(pl.multiple_of(p * width, width), width)

    def up(s, p):
        return pltpu.make_async_remote_copy(
            src_ref=tops.at[s, p], dst_ref=below.at[s, p],
            send_sem=up_send.at[s, p], recv_sem=up_recv.at[s, p],
            device_id={"row": me - 1}, device_id_type=MESH,
        )

    def down(s, p):
        target = back.at[p] if s == 0 else out_ref.at[pl.ds(0, bw), columns(p)]
        return pltpu.make_async_remote_copy(
            src_ref=returned.at[s, p], dst_ref=target,
            send_sem=down_send.at[s, p], recv_sem=down_recv.at[s, p],
            device_id={"row": me + 1}, device_id_type=MESH,
        )

    def sweep(s):
        def piece(p, carry):
            if s == 0:
                x0, x1 = x_ref[:bw, columns(p)], x_ref[bw:, columns(p)]
            else:
                @pl.when(jnp.logical_not(first))
                def _():
                    down(0, p).wait_recv()

                x0, x1 = back[p], middle[p]

            @pl.when(jnp.logical_not(last))
            def _():
                up(s, p).wait_recv()

            parts = split(jnp.concatenate([x0, x1, below[s, p]], axis=0))
            tops[s, p] = dot3((upper_high[s, :bw], upper_low[s, :bw]), parts)

            @pl.when(jnp.logical_not(first))
            def _():
                up(s, p).start()

            tail = tuple(value[bw:] for value in parts)
            returned[s, p] = dot3((lower_high[s], lower_low[s]), tail)

            @pl.when(jnp.logical_not(last))
            def _():
                down(s, p).start()

            kept = dot3((upper_high[s, bw:], upper_low[s, bw:]), parts)
            if s == 0:
                middle[p] = kept

                @pl.when(first)
                def _():
                    back[p] = tops[s, p]
            else:
                out_ref[bw:, columns(p)] = kept

                @pl.when(first)
                def _():
                    out_ref[:bw, columns(p)] = tops[s, p]

            return carry

        lax.fori_loop(0, pieces, piece, 0)

    build(0)
    sweep(0)
    for k in range(1, ring):
        far(k, lax.rem(slab + ring - k, ring)).wait_recv()
    build(1)
    sweep(1)

    for t in range(ring - 1):
        for way in range(2):
            @pl.when(sends(way, t))
            def _():
                hop(way, t, slab).wait_send()

    for k in range(1, ring):
        far(k, slab).wait_send()

    def finish(p, carry):
        @pl.when(jnp.logical_not(first))
        def _():
            up(0, p).wait_send()
            up(1, p).wait_send()
            down(1, p).wait_recv()

        @pl.when(jnp.logical_not(last))
        def _():
            down(0, p).wait_send()
            down(1, p).wait_send()

        return carry

    lax.fori_loop(0, pieces, finish, 0)


def per_device(singular_vectors, reflector_vectors, reflector_factors, sweep_bounds):
    count, ring = lax.axis_size("row"), lax.axis_size("col")
    rows, cols = singular_vectors.shape
    sweeps, blocks, _, span = reflector_vectors.shape
    bw = span // 2
    assert sweeps == 2 and blocks == 2 and rows == span and cols % WIDTH == 0
    pieces = cols // WIDTH
    vmem, dma = pltpu.VMEM, pltpu.SemaphoreType.DMA
    return pl.pallas_call(
        functools.partial(kernel, count, ring),
        out_shape=jax.ShapeDtypeStruct((rows, cols), f32),
        in_specs=[pl.BlockSpec(memory_space=pltpu.SMEM)] + [pl.BlockSpec(memory_space=vmem)] * 3,
        out_specs=pl.BlockSpec(memory_space=vmem),
        scratch_shapes=[
            vmem((2, 2, bw, span), f32),
            vmem((2, span, 3 * bw), bf16), vmem((2, span, 3 * bw), bf16),
            vmem((2, bw, span), bf16), vmem((2, bw, span), bf16),
            vmem((2, pieces, bw, WIDTH), f32),
            vmem((2, pieces, bw, WIDTH), f32),
            vmem((2, pieces, bw, WIDTH), f32),
            vmem((pieces, bw, WIDTH), f32),
            vmem((pieces, bw, WIDTH), f32),
            dma((2, ring)), dma((2, ring)), dma((ring,)), dma((ring,)),
            dma((2, pieces)), dma((2, pieces)), dma((2, pieces)), dma((2, pieces)),
        ],
        compiler_params=pltpu.CompilerParams(
            collective_id=0, has_side_effects=True, vmem_limit_bytes=56 * 2**20
        ),
    )(sweep_bounds, singular_vectors, reflector_vectors, reflector_factors)


def solution(mesh):
    placed = (P("row", "col"), P(None, "row", "col", None), P(None, "row", "col", None), P())
    return jax.shard_map(
        per_device, mesh=mesh, in_specs=placed, out_specs=P("row", "col"), check_vma=False
    )
```

```python
import functools

import jax
import jax.numpy as jnp
from jax import lax
from jax.experimental import pallas as pl
from jax.experimental.pallas import tpu as pltpu
from jax.sharding import PartitionSpec as P

MESH = pl.DeviceIdType.MESH
f32, bf16 = jnp.float32, jnp.bfloat16
WIDTH = 128


def split(value):
    high = value.astype(bf16)
    return high, (value - high.astype(f32)).astype(bf16)


def dot3(a, b):
    (a_high, a_low), (b_high, b_low) = a, b
    dot = functools.partial(jnp.dot, preferred_element_type=f32)
    return dot(a_high, b_high) + (dot(a_high, b_low) + dot(a_low, b_high))


def kernel(
    count, ring, bounds_ref, x_ref, vec_ref, fac_ref, out_ref,
    gathered, upper_high, upper_low, lower_high, lower_low,
    below, tops, returned, back, middle,
    hop_send, hop_recv, up_send, up_recv, down_send, down_recv,
):
    me, slab = lax.axis_index("row"), lax.axis_index("col")
    bw = gathered.shape[2]
    part = bw // ring
    pieces, width = below.shape[1], below.shape[3]
    first, last = me == 0, me == count - 1

    def block_rows(owner):
        return pl.ds(pl.multiple_of(owner * part, part), part)

    for s in range(2):
        for b in range(2):
            w = vec_ref[s, b]
            gathered[s, b, block_rows(slab), :bw] = w[:, :bw] + w[:, bw:]
            gathered[s, b, block_rows(slab), bw:] = fac_ref[s, b]

    @pl.when(last)
    def _():
        below[...] = jnp.zeros_like(below)

    barrier = pltpu.get_barrier_semaphore()

    @pl.when(jnp.logical_not(first))
    def _():
        pl.semaphore_signal(barrier, inc=1, device_id={"row": me - 1}, device_id_type=MESH)

    @pl.when(jnp.logical_not(last))
    def _():
        pl.semaphore_signal(barrier, inc=1, device_id={"row": me + 1}, device_id_type=MESH)

    @pl.when(slab > 0)
    def _():
        pl.semaphore_signal(barrier, inc=1, device_id={"col": slab - 1}, device_id_type=MESH)

    @pl.when(slab < ring - 1)
    def _():
        pl.semaphore_signal(barrier, inc=1, device_id={"col": slab + 1}, device_id_type=MESH)

    peers = jnp.where(me > 0, 1, 0) + jnp.where(me < count - 1, 1, 0)
    peers = peers + jnp.where(slab > 0, 1, 0) + jnp.where(slab < ring - 1, 1, 0)
    pl.semaphore_wait(barrier, peers)

    def hop(s, way, t, owner):
        block = gathered.at[s, :, block_rows(owner)]
        return pltpu.make_async_remote_copy(
            src_ref=block, dst_ref=block,
            send_sem=hop_send.at[s, way, t], recv_sem=hop_recv.at[s, way, t],
            device_id={"col": slab + (1 - 2 * way)}, device_id_type=MESH,
        )

    def sends(way, t):
        if way == 0:
            return (slab - t >= 0) & (slab + 1 < ring)
        return (slab + t < ring) & (slab >= 1)

    def gets(way, t):
        return slab - 1 - t >= 0 if way == 0 else slab + 1 + t < ring

    def start_hops(s, t):
        for way in range(2):
            @pl.when(sends(way, t))
            def _():
                hop(s, way, t, slab - (1 - 2 * way) * t).start()

    def wait_hops(s, t):
        for way in range(2):
            @pl.when(gets(way, t))
            def _():
                hop(s, way, t, slab - (1 - 2 * way) * (t + 1)).wait_recv()

    for t in range(ring - 1):
        for s in range(2):
            if t > 0:
                wait_hops(s, t - 1)
            start_hops(s, t)

    def build(s):
        row = lax.broadcasted_iota(jnp.int32, (bw, bw), 0)
        col = lax.broadcasted_iota(jnp.int32, (bw, bw), 1)
        row2 = lax.broadcasted_iota(jnp.int32, (2 * bw, 2 * bw), 0)
        col2 = lax.broadcasted_iota(jnp.int32, (2 * bw, 2 * bw), 1)
        unit = jnp.where(row2 == col2, 1.0, 0.0).astype(f32)

        def whole(b):
            start = (me * 2 + b) * bw
            live = (start >= bounds_ref[s, 0]) & (start <= bounds_ref[s, 1])
            packed = gathered[s, b, :, :bw]
            factor = gathered[s, b, :, bw:] * jnp.where(live, 1.0, 0.0).astype(f32)
            w_t = jnp.concatenate(
                [jnp.where(col >= row, packed, 0.0), jnp.where(col < row, packed, 0.0)], axis=1
            )
            g = dot3(split(factor), split(w_t))
            return unit - dot3(split(w_t.T), split(g))

        q1 = whole(1)
        lower_high[s], lower_low[s] = split(q1[bw:])
        q0 = whole(0)
        mixed = dot3(split(q0[:, bw:]), split(q1[:bw]))
        upper_high[s, :, :bw], upper_low[s, :, :bw] = split(q0[:, :bw])
        upper_high[s, :, bw:], upper_low[s, :, bw:] = split(mixed)

    def columns(p):
        return pl.ds(pl.multiple_of(p * width, width), width)

    def up(s, p):
        return pltpu.make_async_remote_copy(
            src_ref=tops.at[s, p], dst_ref=below.at[s, p],
            send_sem=up_send.at[s, p], recv_sem=up_recv.at[s, p],
            device_id={"row": me - 1}, device_id_type=MESH,
        )

    def down(s, p):
        target = back.at[p] if s == 0 else out_ref.at[pl.ds(0, bw), columns(p)]
        return pltpu.make_async_remote_copy(
            src_ref=returned.at[s, p], dst_ref=target,
            send_sem=down_send.at[s, p], recv_sem=down_recv.at[s, p],
            device_id={"row": me + 1}, device_id_type=MESH,
        )

    def sweep(s):
        def piece(p, carry):
            if s == 0:
                x0, x1 = x_ref[:bw, columns(p)], x_ref[bw:, columns(p)]
            else:
                @pl.when(jnp.logical_not(first))
                def _():
                    down(0, p).wait_recv()

                x0, x1 = back[p], middle[p]

            @pl.when(jnp.logical_not(last))
            def _():
                up(s, p).wait_recv()

            parts = split(jnp.concatenate([x0, x1, below[s, p]], axis=0))
            tops[s, p] = dot3((upper_high[s, :bw], upper_low[s, :bw]), parts)

            @pl.when(jnp.logical_not(first))
            def _():
                up(s, p).start()

            tail = tuple(value[bw:] for value in parts)
            returned[s, p] = dot3((lower_high[s], lower_low[s]), tail)

            @pl.when(jnp.logical_not(last))
            def _():
                down(s, p).start()

            kept = dot3((upper_high[s, bw:], upper_low[s, bw:]), parts)
            if s == 0:
                middle[p] = kept

                @pl.when(first)
                def _():
                    back[p] = tops[s, p]
            else:
                out_ref[bw:, columns(p)] = kept

                @pl.when(first)
                def _():
                    out_ref[:bw, columns(p)] = tops[s, p]

            return carry

        lax.fori_loop(0, pieces, piece, 0)

    wait_hops(0, ring - 2)
    build(0)
    sweep(0)
    wait_hops(1, ring - 2)
    build(1)
    sweep(1)

    for t in range(ring - 1):
        for way in range(2):
            @pl.when(sends(way, t))
            def _():
                hop(0, way, t, slab).wait_send()
                hop(1, way, t, slab).wait_send()

    def finish(p, carry):
        @pl.when(jnp.logical_not(first))
        def _():
            up(0, p).wait_send()
            up(1, p).wait_send()
            down(1, p).wait_recv()

        @pl.when(jnp.logical_not(last))
        def _():
            down(0, p).wait_send()
            down(1, p).wait_send()

        return carry

    lax.fori_loop(0, pieces, finish, 0)


def per_device(singular_vectors, reflector_vectors, reflector_factors, sweep_bounds):
    count, ring = lax.axis_size("row"), lax.axis_size("col")
    rows, cols = singular_vectors.shape
    sweeps, blocks, _, span = reflector_vectors.shape
    bw = span // 2
    assert sweeps == 2 and blocks == 2 and rows == span and cols % WIDTH == 0
    pieces = cols // WIDTH
    vmem, dma = pltpu.VMEM, pltpu.SemaphoreType.DMA
    return pl.pallas_call(
        functools.partial(kernel, count, ring),
        out_shape=jax.ShapeDtypeStruct((rows, cols), f32),
        in_specs=[pl.BlockSpec(memory_space=pltpu.SMEM)] + [pl.BlockSpec(memory_space=vmem)] * 3,
        out_specs=pl.BlockSpec(memory_space=vmem),
        scratch_shapes=[
            vmem((2, 2, bw, span), f32),
            vmem((2, span, 3 * bw), bf16), vmem((2, span, 3 * bw), bf16),
            vmem((2, bw, span), bf16), vmem((2, bw, span), bf16),
            vmem((2, pieces, bw, WIDTH), f32),
            vmem((2, pieces, bw, WIDTH), f32),
            vmem((2, pieces, bw, WIDTH), f32),
            vmem((pieces, bw, WIDTH), f32),
            vmem((pieces, bw, WIDTH), f32),
            dma((2, 2, ring)), dma((2, 2, ring)),
            dma((2, pieces)), dma((2, pieces)), dma((2, pieces)), dma((2, pieces)),
        ],
        compiler_params=pltpu.CompilerParams(
            collective_id=0, has_side_effects=True, vmem_limit_bytes=56 * 2**20
        ),
    )(sweep_bounds, singular_vectors, reflector_vectors, reflector_factors)


def solution(mesh):
    placed = (P("row", "col"), P(None, "row", "col", None), P(None, "row", "col", None), P())
    return jax.shard_map(
        per_device, mesh=mesh, in_specs=placed, out_specs=P("row", "col"), check_vma=False
    )
```
